512 devices in a mesh: seq: 64 (over x, z), head: 8 (over y, core).
Axes of the slice: x: 4, y: 4, z: 16, core: 2. Of those that a mesh axis runs over, the one named last changes fastest.
Arguments:
- queries: bfloat16 [16384, 4096], P('seq', 'head'), may hold values from -12 to 12
- key_input: bfloat16 [16384, 4096], P('seq', 'head'), may hold values from -1.796875 to 1.796875
- value_input: bfloat16 [16384, 4096], P('seq', 'head'), may hold values from -32 to 32
- norm_gain: bfloat16 [4096], P('head'), may hold values from 0.099609375 to 1.8984375
- out_weight: bfloat16 [4096, 3072], P('head', 'seq'), may hold values from -0.25 to 0.25
- target: bfloat16 [16384, 3072], P('seq', 'head'), may hold values from -6 to 6
Outputs:
- output: bfloat16 [16384, 3072], P('seq', 'head')
- query_grad: bfloat16 [16384, 4096], P('seq', 'head')
- key_grad: bfloat16 [16384, 4096], P('seq', 'head')
- value_grad: bfloat16 [16384, 4096], P('seq', 'head')
- gain_grads: float32 [64, 4096], P('seq', 'head')
- weight_grads: bfloat16 [64, 4096, 3072], P('seq', 'head')
The draws below stay inside these ranges and needn't reach their ends.
All inputs are finite; a program needn't handle non-finite values.
Results may differ from the reference program's by a relative error of at most 0.022.
Values may be sent and summed in bfloat16 or wider, within the bound.
No kernel may reach another device: no remote copies, remote signals or barrier semaphores. Data moves between devices by JAX's collectives and lax.ppermute only.
A program may use at most 64 MiB of HBM per device.

```python
import math
import jax
import jax.numpy as jnp
from jax import lax

TOK_DEV = 256
HEADS = 32
HEAD_DIM = 128
OUT_WIDTH = 3072
FEATURES = 4096
TOKENS = 16384
N_SEQ = 64


def draw_queries(key, part):
    first, second = jax.random.split(jax.random.fold_in(key, 11))
    shape = (TOKENS, HEADS * HEAD_DIM)
    base = jnp.clip(jax.random.normal(first, shape, jnp.float32), -4.0, 4.0)
    spread = jnp.exp(jax.random.uniform(second, (TOKENS, 1), jnp.float32, 0.0, math.log(10.0)))
    return (0.3 * base * spread).astype(jnp.bfloat16)


def draw_value_input(key, part):
    first, second = jax.random.split(jax.random.fold_in(key, 23), 2)
    width = HEADS * HEAD_DIM
    shape = (TOKENS, width)
    ramp = jnp.arange(width, dtype=jnp.float32) / width
    jitter = jax.random.uniform(second, (1, width), jnp.float32, 0.0, math.log(10.0 / 3.0))
    base = jnp.clip(jax.random.normal(first, shape, jnp.float32), -3.0, 3.0)
    column = jnp.exp(math.log(3.0) * ramp[None, :] + jitter)
    return (0.2 * base * column).astype(jnp.bfloat16)


def raised(values, key, source, target, parts, factor):
    owner, partner = [(jnp.arange(values.shape[position]) // (values.shape[position] // parts)).reshape([-1 if axis == position else 1 for axis in range(values.ndim)]) for position in (source, target)]
    chosen = jax.random.permutation(key, parts)[partner]
    strong = (owner == chosen) | (owner == (partner + parts // 2) % parts)
    return jnp.where(strong, factor * values, values)


def block_scale(rng, shape, pieces, least, top_value):
    def one(axis_at, parts):
        steps = jax.random.uniform(jax.random.fold_in(jax.random.fold_in(rng, 6), axis_at), (parts,), jnp.float32, least / len(pieces), top_value / len(pieces))
        return jnp.repeat(jnp.exp(steps), shape[axis_at] // parts).reshape((-1,) + (1,) * (len(shape) - axis_at - 1))

    factor_of = one(*pieces[0])
    for cut in pieces[1:]:
        factor_of = factor_of * one(*cut)
    return factor_of


def gaussian(rng, dims, scale, most, pieces=(), held_as=jnp.bfloat16):
    gain = block_scale(rng, dims, pieces, -0.22, 0.18) if pieces else 1.0
    entries = jax.random.normal(rng, dims, jnp.float32) * scale * gain
    return jnp.minimum(jnp.maximum(entries, -most), most).astype(held_as)


def heavy_noise(rng, shape, scale, reach, cuts, heavy, held_as=jnp.bfloat16):
    array = scale * jax.random.normal(rng, shape, jnp.float32)
    if cuts:
        array = array * block_scale(rng, shape, cuts, -0.22, 0.18)
    return jnp.clip(raised(array, jax.random.fold_in(rng, 3), *heavy), -reach, reach).astype(held_as)


def setup_inputs(seed: int = 0) -> dict:
    key_of = jax.random.split(jax.random.key(seed), 7)
    queries = draw_queries(jax.random.fold_in(key_of[6], 71), 0)
    key_input = gaussian(key_of[1], (TOKENS, FEATURES), 0.3, 1.796875, ((0, 64), (1, 8)))
    value_input = draw_value_input(jax.random.fold_in(key_of[6], 71), 0)
    norm_gain = jnp.clip(1.0 + 0.18 * jax.random.normal(key_of[3], (FEATURES,), jnp.float32), 0.099609375, 1.8984375).astype(jnp.bfloat16)
    out_weight = heavy_noise(key_of[4], (FEATURES, OUT_WIDTH), FEATURES ** -0.5, 0.25, ((0, 8), (1, 64)), (0, 1, 64, 4.0))
    target = gaussian(key_of[5], (TOKENS, OUT_WIDTH), 1.0, 6.0, ((0, 64), (1, 8)))
    return {"queries": queries, "key_input": key_input, "value_input": value_input, "norm_gain": norm_gain, "out_weight": out_weight, "target": target}


EPSILON = 1e-06

def causal(count):
    row_index = lax.broadcasted_iota(jnp.int32, (count, count), 0)
    col_index = lax.broadcasted_iota(jnp.int32, (count, count), 1)
    return row_index >= col_index

def reference(queries, key_input, value_input, norm_gain, out_weight, target):
    shape4 = (N_SEQ, TOK_DEV, HEADS, HEAD_DIM)
    q_all = queries.reshape(shape4)
    k_all = key_input.reshape(shape4)
    v_all = value_input.reshape(shape4)
    keep_mask = causal(TOK_DEV)

    def forward_step(state, inputs):
        q_block, k_block, v_block = inputs
        q_float = q_block.astype(jnp.float32)
        k_float = k_block.astype(jnp.float32)
        v_float = v_block.astype(jnp.float32)
        state_low = state.astype(jnp.bfloat16)
        scores = jnp.einsum('thd,shd->hts', q_float, k_float)
        scores_low = jnp.where(keep_mask[None], scores, 0.0).astype(jnp.bfloat16)
        attended = jnp.einsum('hts,shd->thd', scores_low.astype(jnp.float32), v_float)
        attended = attended + jnp.einsum('thd,hde->the', q_float, state_low.astype(jnp.float32))
        state_next = state + jnp.einsum('shd,she->hde', k_float, v_float)
        return (state_next, (attended, state_low))
    zero_state = jnp.zeros((HEADS, HEAD_DIM, HEAD_DIM), jnp.float32)
    _, (attended, states) = lax.scan(forward_step, zero_state, (q_all, k_all, v_all))
    mixed = attended.reshape(TOKENS, FEATURES)
    gain_float = norm_gain.astype(jnp.float32)
    squares = lax.optimization_barrier(jnp.sum(mixed * mixed, axis=1, keepdims=True))
    inverse = lax.rsqrt(squares / FEATURES + EPSILON)
    normed = (mixed * inverse * gain_float).astype(jnp.bfloat16)
    projected = jnp.dot(normed, out_weight, preferred_element_type=jnp.float32)
    output = projected.astype(jnp.bfloat16)
    out_grad = (projected - target.astype(jnp.float32)).astype(jnp.bfloat16)
    normed_grad = jnp.dot(out_grad, out_weight.T, preferred_element_type=jnp.float32)
    inner = lax.optimization_barrier(jnp.sum(mixed * gain_float * normed_grad, axis=1, keepdims=True))
    mixed_grad = inverse * gain_float * normed_grad - mixed * inverse ** 3 * inner / FEATURES
    mixed_grad = mixed_grad.astype(jnp.bfloat16)
    gain_grads = lax.optimization_barrier(jnp.sum((normed_grad * mixed * inverse).reshape(N_SEQ, TOK_DEV, FEATURES), axis=1))

    def block_weight(pair):
        return lax.dot_general(pair[0], pair[1], (((0,), (0,)), ((), ())), preferred_element_type=jnp.float32).astype(jnp.bfloat16)
    weight_grads = lax.map(block_weight, (normed.reshape(N_SEQ, TOK_DEV, FEATURES), out_grad.reshape(N_SEQ, TOK_DEV, OUT_WIDTH)))
    grad_all = mixed_grad.reshape(shape4)

    def backward_step(later, inputs):
        q_block, k_block, v_block, grad_block, state_low = inputs
        q_float = q_block.astype(jnp.float32)
        k_float = k_block.astype(jnp.float32)
        v_float = v_block.astype(jnp.float32)
        grad_float = grad_block.astype(jnp.float32)
        state_float = state_low.astype(jnp.float32)
        later_float = later.astype(jnp.bfloat16).astype(jnp.float32)
        scores = jnp.einsum('thd,shd->hts', q_float, k_float)
        scores_float = jnp.where(keep_mask[None], scores, 0.0).astype(jnp.bfloat16).astype(jnp.float32)
        pairs = jnp.einsum('thd,shd->hts', grad_float, v_float)
        pairs_float = jnp.where(keep_mask[None], pairs, 0.0).astype(jnp.bfloat16).astype(jnp.float32)
        query_part = jnp.einsum('hts,shd->thd', pairs_float, k_float) + jnp.einsum('the,hde->thd', grad_float, state_float)
        key_part = jnp.einsum('hts,thd->shd', pairs_float, q_float) + jnp.einsum('she,hde->shd', v_float, later_float)
        value_part = jnp.einsum('hts,the->she', scores_float, grad_float) + jnp.einsum('shd,hde->she', k_float, later_float)
        later_next = later + jnp.einsum('thd,the->hde', q_float, grad_float)
        return (later_next, (query_part.astype(jnp.bfloat16), key_part.astype(jnp.bfloat16), value_part.astype(jnp.bfloat16)))
    _, (query_grad, key_grad, value_grad) = lax.scan(backward_step, zero_state, (q_all, k_all, v_all, grad_all, states), reverse=True)
    return (output, query_grad.reshape(TOKENS, FEATURES), key_grad.reshape(TOKENS, FEATURES), value_grad.reshape(TOKENS, FEATURES), gain_grads, weight_grads)
```

```python
import functools

import jax
import jax.numpy as jnp
from jax import lax
from jax.experimental import pallas as pl
from jax.experimental.pallas import tpu as pltpu
from jax.sharding import Mesh
from jax.sharding import PartitionSpec as P

HEAD_DIM = 128
FEATURES = 4096
SEQ = ("x", "z")
HEAD = ("y", "c")
EPSILON = 1e-06
F32 = jnp.float32
BF16 = jnp.bfloat16
NX, NZ, NY, NC = 4, 16, 4, 2
EXTRA = 8


def dot(a, b, ca, cb):
    return lax.dot_general(a, b, (((ca,), (cb,)), ((), ())), preferred_element_type=F32)


def call(kernel, outs, args, flops=0, name=None):
    moved = sum(a.size * a.dtype.itemsize for a in args)
    moved += sum(o.size * o.dtype.itemsize for o in outs)
    return pl.pallas_call(
        kernel,
        out_shape=outs,
        in_specs=[pl.BlockSpec(memory_space=pltpu.VMEM)] * len(args),
        out_specs=[pl.BlockSpec(memory_space=pltpu.VMEM)] * len(outs),
        cost_estimate=pl.CostEstimate(flops=flops, bytes_accessed=moved, transcendentals=0),
        name=name,
    )(*args)


def arr(shape, dtype):
    return jax.ShapeDtypeStruct(shape, dtype)


def head_cols(h):
    return slice(h * HEAD_DIM, (h + 1) * HEAD_DIM)


def keep_mask(count):
    rows = lax.broadcasted_iota(jnp.int32, (count, count), 0)
    cols = lax.broadcasted_iota(jnp.int32, (count, count), 1)
    return rows >= cols


def row_sums(p):
    high = p.astype(BF16)
    low = (p - high.astype(F32)).astype(BF16)
    ones = jnp.ones((EXTRA, p.shape[1]), BF16)
    return dot(ones, high, 1, 1) + dot(ones, low, 1, 1)


def pack_rows(sums):
    high = sums.astype(BF16).astype(F32)
    low = sums - high
    row = lax.broadcasted_iota(jnp.int32, sums.shape, 0)
    return jnp.where(row < EXTRA // 2, high, low).astype(BF16)


def unpack_rows(packed):
    wide = packed.astype(F32)
    return wide[0:1] + wide[EXTRA // 2 : EXTRA // 2 + 1]


def as_columns(row):
    return jnp.broadcast_to(row, (HEAD_DIM, row.shape[1])).T


def state_kernel(a_ref, b_ref, out_ref):
    for h in range(a_ref.shape[1] // HEAD_DIM):
        cols = head_cols(h)
        out_ref[cols, :] = dot(a_ref[:, cols], b_ref[:, cols], 0, 0).astype(BF16)


def local_kernel(q_ref, k_ref, v_ref, out_ref):
    keep = keep_mask(q_ref.shape[0])
    for h in range(q_ref.shape[1] // HEAD_DIM):
        cols = head_cols(h)
        scores = dot(q_ref[:, cols], k_ref[:, cols], 1, 1)
        scores = jnp.where(keep, scores, 0.0).astype(BF16)
        out_ref[:, cols] = dot(scores, v_ref[:, cols], 1, 0)


def totals_kernel(reverse, in_ref, out_ref):
    total = in_ref[0].astype(F32)
    for i in range(1, NZ):
        total = total + in_ref[i].astype(F32)
    x = lax.axis_index("x")
    for k in range(NX):
        sent = (k < x) if reverse else (k > x)
        out_ref[k] = jnp.where(sent, total, 0.0)


def prefix_kernel(reverse, in_ref, offset_ref, out_ref):
    running = offset_ref[0]
    for k in range(1, NX):
        running = running + offset_ref[k]
    order = range(NZ)
    for i in reversed(order) if reverse else order:
        out_ref[i] = running.astype(BF16)
        running = running + in_ref[i].astype(F32)


def project_kernel(
    att_ref, q_ref, state_ref, gain_ref, w0_ref, w1_ref, w3_ref, wa_ref, wb_ref,
    mixed_ref, keep_ref, send_ref, sums_ref,
):
    for h in range(q_ref.shape[1] // HEAD_DIM):
        cols = head_cols(h)
        mixed_ref[:, cols] = att_ref[:, cols] + dot(q_ref[:, cols], state_ref[cols, :], 1, 0)
    mixed = mixed_ref[...]
    scaled = (mixed * gain_ref[...].astype(F32)).astype(BF16)
    sums = row_sums(mixed * mixed)
    sums_ref[...] = sums
    packed = pack_rows(sums)
    x, c = lax.axis_index("x"), lax.axis_index("c")
    count, width = keep_ref.shape[1], keep_ref.shape[2]
    own = pl.ds(pl.multiple_of(c * width, width), width)
    other = pl.ds(pl.multiple_of((1 - c) * width, width), width)
    weights = (
        (w0_ref[own, :], w0_ref[other, :]),
        (w1_ref[own, :], w1_ref[other, :]),
        (wa_ref[...], wb_ref[...]),
        (w3_ref[own, :], w3_ref[other, :]),
    )
    for r, (mine, theirs) in enumerate(weights):
        place = lax.rem(x + r, NX)
        keep_ref[place] = dot(scaled, mine, 1, 1)
        send_ref[place, 0:count, :] = dot(scaled, theirs, 1, 1).astype(BF16)
        send_ref[r, count : count + EXTRA, 0:count] = packed
        send_ref[r, count : count + EXTRA, count:width] = jnp.zeros((EXTRA, width - count), BF16)


def pair_kernel(keep_ref, got_ref, sums_ref, out_ref):
    count, width = keep_ref.shape[1], keep_ref.shape[2]
    sums = sums_ref[...] + unpack_rows(got_ref[0, count : count + EXTRA, 0:count])
    packed = pack_rows(sums)
    for k in range(NY):
        out_ref[k, 0:count, :] = (keep_ref[k] + got_ref[k, 0:count, :].astype(F32)).astype(BF16)
        out_ref[k, count : count + EXTRA, 0:count] = packed
        out_ref[k, count : count + EXTRA, count:width] = jnp.zeros((EXTRA, width - count), BF16)


def output_kernel(got_ref, target_ref, out_ref, grad_ref, inverse_ref):
    count, width = target_ref.shape
    total = got_ref[0, 0:count, :].astype(F32)
    squares = unpack_rows(got_ref[0, count : count + EXTRA, 0:count])
    for k in range(1, NY):
        total = total + got_ref[k, 0:count, :].astype(F32)
        squares = squares + unpack_rows(got_ref[k, count : count + EXTRA, 0:count])
    inverse = lax.rsqrt(squares / FEATURES + EPSILON)
    inverse_ref[...] = jnp.broadcast_to(inverse, inverse_ref.shape)
    scale = as_columns(inverse)
    projected = total * jnp.concatenate([scale] * (width // HEAD_DIM), axis=1)
    out_ref[...] = projected.astype(BF16)
    grad = (projected - target_ref[...].astype(F32)).astype(BF16)
    grad_ref[0:count, :] = grad
    packed = pack_rows(row_sums(grad.astype(F32) * projected))
    grad_ref[count : count + EXTRA, 0:count] = packed
    grad_ref[count : count + EXTRA, count:width] = jnp.zeros((EXTRA, width - count), BF16)


def mixed_grad_kernel(
    own_ref, other_ref, w0_ref, w1_ref, w3_ref, wa_ref, wb_ref, mixed_ref, gain_ref, inverse_ref,
    q_ref, grad_ref, gain_grad_ref, state_ref,
):
    count = mixed_ref.shape[0]
    width = own_ref.shape[2]
    x, c = lax.axis_index("x"), lax.axis_index("c")
    own = pl.ds(pl.multiple_of(c * width, width), width)
    other = pl.ds(pl.multiple_of((1 - c) * width, width), width)
    weights = (
        (w0_ref[own, :], w0_ref[other, :]),
        (w1_ref[own, :], w1_ref[other, :]),
        (wa_ref[...], wb_ref[...]),
        (w3_ref[own, :], w3_ref[other, :]),
    )
    total = None
    for r, (mine, theirs) in enumerate(weights):
        place = lax.rem(x + r, NX)
        part = dot(own_ref[place, 0:count, :], mine, 1, 0)
        part = part + dot(other_ref[place, 0:count, :], theirs, 1, 0)
        total = part if total is None else total + part
    inner = None
    for ref in (own_ref, other_ref):
        for k in range(NY):
            piece = unpack_rows(ref[k, count : count + EXTRA, 0:count])
            inner = piece if inner is None else inner + piece
    inverse = inverse_ref[0:1, :]
    slope = inverse * inverse * inner / FEATURES
    heads = mixed_ref.shape[1] // HEAD_DIM
    scale = jnp.concatenate([as_columns(inverse)] * heads, axis=1)
    slope = jnp.concatenate([as_columns(slope)] * heads, axis=1)
    mixed = mixed_ref[...]
    scaled = scale * total
    grad = (gain_ref[...].astype(F32) * scaled - mixed * slope).astype(BF16)
    grad_ref[...] = grad
    gain_grad_ref[...] = jnp.sum(scaled * mixed, axis=0, keepdims=True)
    for h in range(heads):
        cols = head_cols(h)
        state_ref[cols, :] = dot(q_ref[:, cols], grad[:, cols], 0, 0).astype(BF16)


def weight_grad_kernel(own_ref, other_ref, mixed_ref, gain_ref, inverse_ref, out_ref):
    count = mixed_ref.shape[0]
    width = own_ref.shape[2]
    heads = mixed_ref.shape[1] // HEAD_DIM
    scale = jnp.concatenate([as_columns(inverse_ref[0:1, :])] * heads, axis=1)
    normed = (mixed_ref[...] * scale * gain_ref[...].astype(F32)).astype(BF16)
    turned = normed.T
    c = lax.axis_index("c")
    for k in range(NY):
        for ref, half in ((own_ref, c), (other_ref, 1 - c)):
            start = pl.multiple_of(k * NC * width + half * width, HEAD_DIM)
            out_ref[0, :, pl.ds(start, width)] = dot(turned, ref[k, 0:count, :], 1, 0).astype(BF16)


def local_grad_kernel(
    q_ref, k_ref, v_ref, grad_ref, state_ref, query_ref, key_ref, value_ref
):
    keep = keep_mask(q_ref.shape[0])
    for h in range(q_ref.shape[1] // HEAD_DIM):
        cols = head_cols(h)
        q, k, v, grad = q_ref[:, cols], k_ref[:, cols], v_ref[:, cols], grad_ref[:, cols]
        scores = jnp.where(keep, dot(q, k, 1, 1), 0.0).astype(BF16)
        pairs = jnp.where(keep, dot(grad, v, 1, 1), 0.0).astype(BF16)
        query = dot(pairs, k, 1, 0) + dot(grad, state_ref[cols, :], 1, 1)
        query_ref[:, cols] = query.astype(BF16)
        key_ref[:, cols] = dot(pairs, q, 0, 0)
        value_ref[:, cols] = dot(scores, grad, 0, 0)


def later_kernel(k_ref, v_ref, key_part_ref, value_part_ref, later_ref, key_ref, value_ref):
    for h in range(k_ref.shape[1] // HEAD_DIM):
        cols = head_cols(h)
        later = later_ref[cols, :]
        key_ref[:, cols] = (key_part_ref[:, cols] + dot(v_ref[:, cols], later, 1, 1)).astype(BF16)
        value = value_part_ref[:, cols] + dot(k_ref[:, cols], later, 1, 0)
        value_ref[:, cols] = value.astype(BF16)


def carried(state, reverse):
    rows, cols = state.shape
    blocks = state.reshape(NZ, rows // NZ, cols)
    got = lax.all_to_all(blocks, "z", 0, 0, tiled=True)
    (totals,) = call(
        functools.partial(totals_kernel, reverse),
        [arr((NX, rows // NZ, cols), F32)], [got], name="totals",
    )
    offsets = lax.all_to_all(totals, "x", 0, 0, tiled=True)
    (sums,) = call(
        functools.partial(prefix_kernel, reverse),
        [arr(blocks.shape, BF16)], [got, offsets], name="prefix",
    )
    return lax.all_to_all(sums, "z", 0, 0, tiled=True).reshape(rows, cols)


def ring(count, step):
    return [(i, (i + step) % count) for i in range(count)]


def per_device(queries, key_input, value_input, norm_gain, out_weight, target):
    count, feats = queries.shape
    width = target.shape[1]
    swap = [(0, 1), (1, 0)]
    gain = norm_gain.reshape(1, feats)
    mm = 2 * count * feats

    (state_local,) = call(
        state_kernel, [arr((feats, HEAD_DIM), BF16)], [key_input, value_input],
        mm * HEAD_DIM, "state",
    )
    w0 = lax.all_gather(out_weight.T, "z", axis=0, tiled=True)
    w3 = lax.ppermute(w0, "x", ring(NX, 1))
    w1 = lax.ppermute(w0, "x", ring(NX, -1))
    c = lax.axis_index("c")
    wa = lax.ppermute(lax.dynamic_slice_in_dim(w3, c * width, width), "x", ring(NX, 1))
    wb = lax.ppermute(lax.dynamic_slice_in_dim(w1, (1 - c) * width, width), "x", ring(NX, -1))
    weights = [w0, w1, w3, wa, wb]

    (attended,) = call(
        local_kernel, [arr((count, feats), F32)], [queries, key_input, value_input],
        2 * mm * count, "local",
    )
    state_low = carried(state_local, False)
    message = (NY, count + EXTRA, width)
    mixed, kept, sent, sums = call(
        project_kernel,
        [
            arr((count, feats), F32),
            arr((NY, count, width), F32),
            arr(message, BF16),
            arr((EXTRA, count), F32),
        ],
        [attended, queries, state_low, gain, *weights],
        mm * (HEAD_DIM + NY * NC * width), "project",
    )
    got = lax.ppermute(sent, "c", swap)
    (paired,) = call(pair_kernel, [arr(message, BF16)], [kept, got, sums], name="pair")
    arrived = lax.all_to_all(paired, "y", 0, 0, tiled=True)
    output, grad_local, inverse = call(
        output_kernel,
        [
            arr((count, width), BF16),
            arr((count + EXTRA, width), BF16),
            arr((EXTRA, count), F32),
        ],
        [arrived, target], name="output",
    )
    own = lax.all_gather(grad_local, "y", axis=0, tiled=True).reshape(message)
    other = lax.ppermute(own, "c", swap)
    mixed_grad, gain_grads, grad_state = call(
        mixed_grad_kernel,
        [arr((count, feats), BF16), arr((1, feats), F32), arr((feats, HEAD_DIM), BF16)],
        [own, other, *weights, mixed, gain, inverse, queries],
        mm * (HEAD_DIM + NY * NC * width), "mixed_grad",
    )
    (weight_grads,) = call(
        weight_grad_kernel, [arr((1, feats, NY * NC * width), BF16)],
        [own, other, mixed, gain, inverse], mm * NY * NC * width, "weight_grad",
    )
    query_grad, key_part, value_part = call(
        local_grad_kernel,
        [arr((count, feats), BF16), arr((count, feats), F32), arr((count, feats), F32)],
        [queries, key_input, value_input, mixed_grad, state_low],
        mm * (5 * count + HEAD_DIM), "local_grad",
    )
    later_low = carried(grad_state, True)
    key_grad, value_grad = call(
        later_kernel, [arr((count, feats), BF16)] * 2,
        [key_input, value_input, key_part, value_part, later_low], 2 * mm * HEAD_DIM, "later",
    )
    return output, query_grad, key_grad, value_grad, gain_grads, weight_grads


def solution(mesh):
    torus = Mesh(mesh.devices.reshape(NX, NZ, NY, NC), ("x", "z", "y", "c"))
    return jax.shard_map(
        per_device,
        mesh=torus,
        in_specs=(
            P(SEQ, HEAD),
            P(SEQ, HEAD),
            P(SEQ, HEAD),
            P(HEAD),
            P(HEAD, SEQ),
            P(SEQ, HEAD),
        ),
        out_specs=(
            P(SEQ, HEAD),
            P(SEQ, HEAD),
            P(SEQ, HEAD),
            P(SEQ, HEAD),
            P(SEQ, HEAD),
            P(SEQ, HEAD, None),
        ),
        check_vma=False,
    )
```

```python
import functools

import jax
import jax.numpy as jnp
from jax import lax
from jax.experimental import pallas as pl
from jax.experimental.pallas import tpu as pltpu
from jax.sharding import Mesh
from jax.sharding import PartitionSpec as P


HEAD_DIM = 128
FEATURES = 4096
SEQ = ("x", "z")
HEAD = ("y", "c")
EPSILON = 1e-06
F32 = jnp.float32
BF16 = jnp.bfloat16
NX, NZ, NY, NC = 4, 16, 4, 2
VMEM_LIMIT = 16 << 20
EXTRA = 8


def dot(a, b, ca, cb):
    return lax.dot_general(a, b, (((ca,), (cb,)), ((), ())), preferred_element_type=F32)


def call(kernel, outs, args, flops=0):
    moved = sum(a.size * a.dtype.itemsize for a in args)
    moved += sum(o.size * o.dtype.itemsize for o in outs)
    return pl.pallas_call(
        kernel,
        out_shape=outs,
        in_specs=[pl.BlockSpec(memory_space=pltpu.VMEM)] * len(args),
        out_specs=[pl.BlockSpec(memory_space=pltpu.VMEM)] * len(outs),
        cost_estimate=pl.CostEstimate(flops=flops, bytes_accessed=moved, transcendentals=0),
        compiler_params=pltpu.CompilerParams(vmem_limit_bytes=VMEM_LIMIT),
    )(*args)


def arr(shape, dtype):
    return jax.ShapeDtypeStruct(shape, dtype)


def head_cols(h):
    return slice(h * HEAD_DIM, (h + 1) * HEAD_DIM)


def keep_mask(count):
    rows = lax.broadcasted_iota(jnp.int32, (count, count), 0)
    cols = lax.broadcasted_iota(jnp.int32, (count, count), 1)
    return rows >= cols


def row_sums(p):
    high = p.astype(BF16)
    low = (p - high.astype(F32)).astype(BF16)
    ones = jnp.ones((EXTRA, p.shape[1]), BF16)
    return dot(ones, high, 1, 1) + dot(ones, low, 1, 1)


def pack_rows(sums):
    high = sums.astype(BF16).astype(F32)
    low = sums - high
    row = lax.broadcasted_iota(jnp.int32, sums.shape, 0)
    return jnp.where(row < EXTRA // 2, high, low).astype(BF16)


def unpack_rows(packed):
    wide = packed.astype(F32)
    return wide[0:1] + wide[EXTRA // 2 : EXTRA // 2 + 1]


def as_columns(row):
    return jnp.broadcast_to(row, (HEAD_DIM, row.shape[1])).T


def state_kernel(a_ref, b_ref, out_ref):
    for h in range(a_ref.shape[1] // HEAD_DIM):
        cols = head_cols(h)
        out_ref[cols, :] = dot(a_ref[:, cols], b_ref[:, cols], 0, 0).astype(BF16)


def local_kernel(q_ref, k_ref, v_ref, out_ref):
    keep = keep_mask(q_ref.shape[0])
    for h in range(q_ref.shape[1] // HEAD_DIM):
        cols = head_cols(h)
        scores = dot(q_ref[:, cols], k_ref[:, cols], 1, 1)
        scores = jnp.where(keep, scores, 0.0).astype(BF16)
        out_ref[:, cols] = dot(scores, v_ref[:, cols], 1, 0)


def totals_kernel(reverse, in_ref, out_ref):
    total = in_ref[0].astype(F32)
    for i in range(1, NZ):
        total = total + in_ref[i].astype(F32)
    x = lax.axis_index("x")
    for k in range(NX):
        sent = (k < x) if reverse else (k > x)
        out_ref[k] = jnp.where(sent, total, 0.0)


def prefix_kernel(reverse, in_ref, offset_ref, out_ref):
    running = offset_ref[0]
    for k in range(1, NX):
        running = running + offset_ref[k]
    order = range(NZ)
    for i in reversed(order) if reverse else order:
        out_ref[i] = running.astype(BF16)
        running = running + in_ref[i].astype(F32)


def halves(refs, c, width):
    w0_ref, w1_ref, w3_ref, wa_ref, wb_ref = refs
    own = pl.ds(pl.multiple_of(c * width, width), width)
    other = pl.ds(pl.multiple_of((1 - c) * width, width), width)
    first, second = wa_ref[...], wb_ref[...]
    return (
        (lambda: w0_ref[own, :], lambda: w0_ref[other, :]),
        (lambda: w1_ref[own, :], lambda: w1_ref[other, :]),
        (lambda: jnp.where(c == 0, first, second), lambda: jnp.where(c == 0, second, first)),
        (lambda: w3_ref[own, :], lambda: w3_ref[other, :]),
    )


def project_kernel(
    att_ref, q_ref, state_ref, gain_ref, w0_ref, w1_ref, w3_ref, wa_ref, wb_ref,
    mixed_ref, scaled_ref, send_ref, sums_ref,
):
    for h in range(q_ref.shape[1] // HEAD_DIM):
        cols = head_cols(h)
        mixed_ref[:, cols] = att_ref[:, cols] + dot(q_ref[:, cols], state_ref[cols, :], 1, 0)
    mixed = mixed_ref[...]
    scaled = (mixed * gain_ref[...].astype(F32)).astype(BF16)
    scaled_ref[...] = scaled
    sums = row_sums(mixed * mixed)
    sums_ref[...] = sums
    packed = pack_rows(sums)
    x, c = lax.axis_index("x"), lax.axis_index("c")
    count, width = mixed.shape[0], send_ref.shape[2]
    for r, (_, theirs) in enumerate(halves((w0_ref, w1_ref, w3_ref, wa_ref, wb_ref), c, width)):
        place = lax.rem(x + r, NX)
        send_ref[place, 0:count, :] = dot(scaled, theirs(), 1, 1).astype(BF16)
        send_ref[r, count : count + EXTRA, 0:count] = packed
        send_ref[r, count : count + EXTRA, count:width] = jnp.zeros((EXTRA, width - count), BF16)


def project_own_kernel(scaled_ref, w0_ref, w1_ref, w3_ref, wa_ref, wb_ref, keep_ref):
    x, c = lax.axis_index("x"), lax.axis_index("c")
    width = keep_ref.shape[2]
    scaled = scaled_ref[...]
    for r, (mine, _) in enumerate(halves((w0_ref, w1_ref, w3_ref, wa_ref, wb_ref), c, width)):
        keep_ref[lax.rem(x + r, NX)] = dot(scaled, mine(), 1, 1)


def pair_kernel(keep_ref, got_ref, sums_ref, out_ref):
    count, width = keep_ref.shape[1], keep_ref.shape[2]
    sums = sums_ref[...] + unpack_rows(got_ref[0, count : count + EXTRA, 0:count])
    packed = pack_rows(sums)
    for k in range(NY):
        out_ref[k, 0:count, :] = (keep_ref[k] + got_ref[k, 0:count, :].astype(F32)).astype(BF16)
        out_ref[k, count : count + EXTRA, 0:count] = packed
        out_ref[k, count : count + EXTRA, count:width] = jnp.zeros((EXTRA, width - count), BF16)


def output_kernel(got_ref, target_ref, out_ref, grad_ref, inverse_ref):
    count, width = target_ref.shape
    total = got_ref[0, 0:count, :].astype(F32)
    squares = unpack_rows(got_ref[0, count : count + EXTRA, 0:count])
    for k in range(1, NY):
        total = total + got_ref[k, 0:count, :].astype(F32)
        squares = squares + unpack_rows(got_ref[k, count : count + EXTRA, 0:count])
    inverse = lax.rsqrt(squares / FEATURES + EPSILON)
    inverse_ref[...] = jnp.broadcast_to(inverse, inverse_ref.shape)
    scale = as_columns(inverse)
    projected = total * jnp.concatenate([scale] * (width // HEAD_DIM), axis=1)
    out_ref[...] = projected.astype(BF16)
    grad = (projected - target_ref[...].astype(F32)).astype(BF16)
    grad_ref[0:count, :] = grad
    packed = pack_rows(row_sums(grad.astype(F32) * projected))
    grad_ref[count : count + EXTRA, 0:count] = packed
    grad_ref[count : count + EXTRA, count:width] = jnp.zeros((EXTRA, width - count), BF16)


def normed_grad_kernel(
    core, grad_ref, w0_ref, w1_ref, w3_ref, wa_ref, wb_ref, out_ref, inner_ref
):
    count, width = out_ref.shape[0], grad_ref.shape[2]
    x, c = lax.axis_index("x"), lax.axis_index("c")
    total = None
    for r, pair in enumerate(halves((w0_ref, w1_ref, w3_ref, wa_ref, wb_ref), c, width)):
        part = dot(grad_ref[lax.rem(x + r, NX), 0:count, :], pair[core](), 1, 0)
        total = part if total is None else total + part
    out_ref[...] = total
    inner = unpack_rows(grad_ref[0, count : count + EXTRA, 0:count])
    for k in range(1, NY):
        inner = inner + unpack_rows(grad_ref[k, count : count + EXTRA, 0:count])
    inner_ref[...] = jnp.broadcast_to(inner, inner_ref.shape)


def mixed_grad_kernel(
    part_ref, part_inner_ref, other_ref, w0_ref, w1_ref, w3_ref, wa_ref, wb_ref,
    mixed_ref, gain_ref, inverse_ref, q_ref, grad_ref, gain_grad_ref, state_ref,
):
    count = mixed_ref.shape[0]
    width = other_ref.shape[2]
    x, c = lax.axis_index("x"), lax.axis_index("c")
    total = part_ref[...]
    for r, (_, theirs) in enumerate(halves((w0_ref, w1_ref, w3_ref, wa_ref, wb_ref), c, width)):
        total = total + dot(other_ref[lax.rem(x + r, NX), 0:count, :], theirs(), 1, 0)
    inner = part_inner_ref[0:1, :]
    for k in range(NY):
        inner = inner + unpack_rows(other_ref[k, count : count + EXTRA, 0:count])
    inverse = inverse_ref[0:1, :]
    slope = inverse * inverse * inner / FEATURES
    heads = mixed_ref.shape[1] // HEAD_DIM
    scale = jnp.concatenate([as_columns(inverse)] * heads, axis=1)
    slope = jnp.concatenate([as_columns(slope)] * heads, axis=1)
    mixed = mixed_ref[...]
    scaled = scale * total
    grad = (gain_ref[...].astype(F32) * scaled - mixed * slope).astype(BF16)
    grad_ref[...] = grad
    gain_grad_ref[...] = jnp.sum(scaled * mixed, axis=0, keepdims=True)
    for h in range(heads):
        cols = head_cols(h)
        state_ref[cols, :] = dot(q_ref[:, cols], grad[:, cols], 0, 0).astype(BF16)


def weight_grad_kernel(own_ref, other_ref, mixed_ref, gain_ref, inverse_ref, out_ref):
    count = mixed_ref.shape[0]
    width = own_ref.shape[2]
    heads = mixed_ref.shape[1] // HEAD_DIM
    scale = jnp.concatenate([as_columns(inverse_ref[0:1, :])] * heads, axis=1)
    normed = (mixed_ref[...] * scale * gain_ref[...].astype(F32)).astype(BF16)
    turned = normed.T
    c = lax.axis_index("c")
    for k in range(NY):
        for ref, half in ((own_ref, c), (other_ref, 1 - c)):
            start = pl.multiple_of(k * NC * width + half * width, HEAD_DIM)
            out_ref[0, :, pl.ds(start, width)] = dot(turned, ref[k, 0:count, :], 1, 0).astype(BF16)


def local_grad_kernel(
    q_ref, k_ref, v_ref, grad_ref, state_ref, scores_ref, query_ref, key_ref, value_ref
):
    keep = keep_mask(q_ref.shape[0])
    for h in range(q_ref.shape[1] // HEAD_DIM):
        cols = head_cols(h)
        q, k, v, grad = q_ref[:, cols], k_ref[:, cols], v_ref[:, cols], grad_ref[:, cols]
        scores = scores_ref[h]
        pairs = jnp.where(keep, dot(grad, v, 1, 1), 0.0).astype(BF16)
        query = dot(pairs, k, 1, 0) + dot(grad, state_ref[cols, :], 1, 1)
        query_ref[:, cols] = query.astype(BF16)
        key_ref[:, cols] = dot(pairs, q, 0, 0)
        value_ref[:, cols] = dot(scores, grad, 0, 0)


def later_kernel(k_ref, v_ref, key_part_ref, value_part_ref, later_ref, key_ref, value_ref):
    for h in range(k_ref.shape[1] // HEAD_DIM):
        cols = head_cols(h)
        later = later_ref[cols, :]
        key_ref[:, cols] = (key_part_ref[:, cols] + dot(v_ref[:, cols], later, 1, 1)).astype(BF16)
        value = value_part_ref[:, cols] + dot(k_ref[:, cols], later, 1, 0)
        value_ref[:, cols] = value.astype(BF16)


def scores_kernel(q_ref, k_ref, out_ref):
    keep = keep_mask(q_ref.shape[0])
    for h in range(q_ref.shape[1] // HEAD_DIM):
        cols = head_cols(h)
        scores = dot(q_ref[:, cols], k_ref[:, cols], 1, 1)
        out_ref[h] = jnp.where(keep, scores, 0.0).astype(BF16)


def exchanged(blocks, axis):
    return lax.all_to_all(blocks, axis, 0, 0, tiled=True)


def carried(state, reverse):
    rows, cols = state.shape
    blocks = state.reshape(NZ, rows // NZ, cols)
    got = exchanged(blocks, "z")
    (totals,) = call(
        functools.partial(totals_kernel, reverse),
        [arr((NX, rows // NZ, cols), F32)], [got],
    )
    offsets = exchanged(totals, "x")
    (sums,) = call(
        functools.partial(prefix_kernel, reverse),
        [arr(blocks.shape, BF16)], [got, offsets],
    )
    return exchanged(sums, "z").reshape(rows, cols)


def ring(count, step):
    return [(i, (i + step) % count) for i in range(count)]


def work(queries, key_input, value_input, norm_gain, out_weight, target):
    count, feats = queries.shape
    width = target.shape[1]
    swap = [(0, 1), (1, 0)]
    gain = norm_gain.reshape(1, feats)
    mm = 2 * count * feats

    (state_local,) = call(
        state_kernel, [arr((feats, HEAD_DIM), BF16)], [key_input, value_input],
        mm * HEAD_DIM,
    )
    w0 = lax.all_gather(out_weight.T, "z", axis=0, tiled=True)
    w3 = lax.ppermute(w0, "x", ring(NX, 1))
    w1 = lax.ppermute(w0, "x", ring(NX, -1))
    wa = lax.ppermute(w3[:width], "x", ring(NX, 1))
    wb = lax.ppermute(w1[width:], "x", ring(NX, -1))
    weights = [w0, w1, w3, wa, wb]

    (attended,) = call(
        local_kernel, [arr((count, feats), F32)], [queries, key_input, value_input],
        2 * mm * count,
    )
    state_low = carried(state_local, False)
    message = (NY, count + EXTRA, width)
    columns = NY * NC * width
    mixed, scaled, sent, sums = call(
        project_kernel,
        [
            arr((count, feats), F32),
            arr((count, feats), BF16),
            arr(message, BF16),
            arr((EXTRA, count), F32),
        ],
        [attended, queries, state_low, gain, *weights],
        mm * (HEAD_DIM + columns // 2),
    )
    (kept,) = call(
        project_own_kernel, [arr((NY, count, width), F32)], [scaled, *weights],
        mm * columns // 2,
    )
    got = lax.ppermute(sent, "c", swap)
    (paired,) = call(pair_kernel, [arr(message, BF16)], [kept, got, sums])
    arrived = exchanged(paired, "y")
    (scores,) = call(
        scores_kernel, [arr((feats // HEAD_DIM, count, count), BF16)], [queries, key_input],
        mm * count,
    )
    output, grad_local, inverse = call(
        output_kernel,
        [
            arr((count, width), BF16),
            arr((count + EXTRA, width), BF16),
            arr((EXTRA, count), F32),
        ],
        [arrived, target],
    )
    own = lax.all_gather(grad_local, "y", axis=0, tiled=True).reshape(message)
    other = lax.ppermute(own, "c", swap)
    part, part_inner = call(
        functools.partial(normed_grad_kernel, 0),
        [arr((count, feats), F32), arr((EXTRA, count), F32)], [own, *weights],
        mm * columns // 2,
    )
    mixed_grad, gain_grads, grad_state = call(
        mixed_grad_kernel,
        [arr((count, feats), BF16), arr((1, feats), F32), arr((feats, HEAD_DIM), BF16)],
        [part, part_inner, other, *weights, mixed, gain, inverse, queries],
        mm * (HEAD_DIM + columns // 2),
    )
    (weight_grads,) = call(
        weight_grad_kernel, [arr((1, feats, columns), BF16)],
        [own, other, mixed, gain, inverse], mm * columns,
    )
    query_grad, key_part, value_part = call(
        local_grad_kernel,
        [arr((count, feats), BF16), arr((count, feats), F32), arr((count, feats), F32)],
        [queries, key_input, value_input, mixed_grad, state_low, scores],
        mm * (4 * count + HEAD_DIM),
    )
    later_low = carried(grad_state, True)
    key_grad, value_grad = call(
        later_kernel, [arr((count, feats), BF16)] * 2,
        [key_input, value_input, key_part, value_part, later_low], 2 * mm * HEAD_DIM,
    )
    return output, query_grad, key_grad, value_grad, gain_grads, weight_grads


def solution(mesh):
    torus = Mesh(mesh.devices.reshape(NX, NZ, NY, NC), ("x", "z", "y", "c"))
    return jax.shard_map(
        work,
        mesh=torus,
        in_specs=(
            P(SEQ, HEAD),
            P(SEQ, HEAD),
            P(SEQ, HEAD),
            P(HEAD),
            P(HEAD, SEQ),
            P(SEQ, HEAD),
        ),
        out_specs=(
            P(SEQ, HEAD),
            P(SEQ, HEAD),
            P(SEQ, HEAD),
            P(SEQ, HEAD),
            P(SEQ, HEAD),
            P(SEQ, HEAD, None),
        ),
        check_vma=False,
    )
```

```python
import functools

import jax
import jax.numpy as jnp
from jax import lax
from jax.experimental import pallas as pl
from jax.experimental.pallas import tpu as pltpu
from jax.sharding import Mesh
from jax.sharding import PartitionSpec as P


HEAD_DIM = 128
FEATURES = 4096
SEQ = ("x", "z")
HEAD = ("y", "c")
EPSILON = 1e-06
F32 = jnp.float32
BF16 = jnp.bfloat16
NX, NZ, NY, NC = 4, 16, 4, 2
VMEM_LIMIT = 16 << 20
EXTRA = 8


def dot(a, b, ca, cb):
    return lax.dot_general(a, b, (((ca,), (cb,)), ((), ())), preferred_element_type=F32)


def call(kernel, outs, args, flops=0, vmem=VMEM_LIMIT):
    moved = sum(a.size * a.dtype.itemsize for a in args)
    moved += sum(o.size * o.dtype.itemsize for o in outs)
    return pl.pallas_call(
        kernel,
        out_shape=outs,
        in_specs=[pl.BlockSpec(memory_space=pltpu.VMEM)] * len(args),
        out_specs=[pl.BlockSpec(memory_space=pltpu.VMEM)] * len(outs),
        cost_estimate=pl.CostEstimate(flops=flops, bytes_accessed=moved, transcendentals=0),
        compiler_params=pltpu.CompilerParams(vmem_limit_bytes=vmem),
    )(*args)


def arr(shape, dtype):
    return jax.ShapeDtypeStruct(shape, dtype)


def head_cols(h):
    return slice(h * HEAD_DIM, (h + 1) * HEAD_DIM)


def keep_mask(count):
    rows = lax.broadcasted_iota(jnp.int32, (count, count), 0)
    cols = lax.broadcasted_iota(jnp.int32, (count, count), 1)
    return rows >= cols


def row_sums(p):
    high = p.astype(BF16)
    low = (p - high.astype(F32)).astype(BF16)
    ones = jnp.ones((EXTRA, p.shape[1]), BF16)
    return dot(ones, high, 1, 1) + dot(ones, low, 1, 1)


def pack_rows(sums):
    high = sums.astype(BF16).astype(F32)
    low = sums - high
    row = lax.broadcasted_iota(jnp.int32, sums.shape, 0)
    return jnp.where(row < EXTRA // 2, high, low).astype(BF16)


def unpack_rows(packed):
    wide = packed.astype(F32)
    return wide[0:1] + wide[EXTRA // 2 : EXTRA // 2 + 1]


def as_columns(row):
    return jnp.broadcast_to(row, (HEAD_DIM, row.shape[1])).T


def state_kernel(a_ref, b_ref, out_ref):
    for h in range(a_ref.shape[1] // HEAD_DIM):
        cols = head_cols(h)
        out_ref[cols, :] = dot(a_ref[:, cols], b_ref[:, cols], 0, 0).astype(BF16)


def local_kernel(q_ref, k_ref, v_ref, out_ref):
    keep = keep_mask(q_ref.shape[0])
    for h in range(q_ref.shape[1] // HEAD_DIM):
        cols = head_cols(h)
        scores = dot(q_ref[:, cols], k_ref[:, cols], 1, 1)
        scores = jnp.where(keep, scores, 0.0).astype(BF16)
        out_ref[:, cols] = dot(scores, v_ref[:, cols], 1, 0)


def totals_kernel(reverse, in_ref, out_ref):
    total = in_ref[0].astype(F32)
    for i in range(1, NZ):
        total = total + in_ref[i].astype(F32)
    x = lax.axis_index("x")
    for k in range(NX):
        sent = (k < x) if reverse else (k > x)
        out_ref[k] = jnp.where(sent, total, 0.0)


def prefix_kernel(reverse, in_ref, offset_ref, out_ref):
    running = offset_ref[0]
    for k in range(1, NX):
        running = running + offset_ref[k]
    order = range(NZ)
    for i in reversed(order) if reverse else order:
        out_ref[i] = running.astype(BF16)
        running = running + in_ref[i].astype(F32)


def halves(refs, c, width):
    w0_ref, w1_ref, w3_ref, wa_ref, wb_ref = refs
    own = pl.ds(pl.multiple_of(c * width, width), width)
    other = pl.ds(pl.multiple_of((1 - c) * width, width), width)
    first, second = wa_ref[...], wb_ref[...]
    return (
        (lambda: w0_ref[own, :], lambda: w0_ref[other, :]),
        (lambda: w1_ref[own, :], lambda: w1_ref[other, :]),
        (lambda: jnp.where(c == 0, first, second), lambda: jnp.where(c == 0, second, first)),
        (lambda: w3_ref[own, :], lambda: w3_ref[other, :]),
    )


def project_kernel(
    att_ref, q_ref, state_ref, gain_ref, w0_ref, w1_ref, w3_ref, wa_ref, wb_ref,
    mixed_ref, scaled_ref, send_ref, sums_ref,
):
    for h in range(q_ref.shape[1] // HEAD_DIM):
        cols = head_cols(h)
        mixed_ref[:, cols] = att_ref[:, cols] + dot(q_ref[:, cols], state_ref[cols, :], 1, 0)
    mixed = mixed_ref[...]
    scaled = (mixed * gain_ref[...].astype(F32)).astype(BF16)
    scaled_ref[...] = scaled
    sums = row_sums(mixed * mixed)
    sums_ref[...] = sums
    packed = pack_rows(sums)
    x, c = lax.axis_index("x"), lax.axis_index("c")
    count, width = mixed.shape[0], send_ref.shape[2]
    for r, (_, theirs) in enumerate(halves((w0_ref, w1_ref, w3_ref, wa_ref, wb_ref), c, width)):
        place = lax.rem(x + r, NX)
        send_ref[place, 0:count, :] = dot(scaled, theirs(), 1, 1).astype(BF16)
        send_ref[r, count : count + EXTRA, 0:count] = packed
        send_ref[r, count : count + EXTRA, count:width] = jnp.zeros((EXTRA, width - count), BF16)


def project_own_kernel(scaled_ref, w0_ref, w1_ref, w3_ref, wa_ref, wb_ref, keep_ref):
    x, c = lax.axis_index("x"), lax.axis_index("c")
    width = keep_ref.shape[2]
    scaled = scaled_ref[...]
    for r, (mine, _) in enumerate(halves((w0_ref, w1_ref, w3_ref, wa_ref, wb_ref), c, width)):
        keep_ref[lax.rem(x + r, NX)] = dot(scaled, mine(), 1, 1)


def pair_kernel(keep_ref, got_ref, sums_ref, out_ref):
    count, width = keep_ref.shape[1], keep_ref.shape[2]
    sums = sums_ref[...] + unpack_rows(got_ref[0, count : count + EXTRA, 0:count])
    packed = pack_rows(sums)
    for k in range(NY):
        out_ref[k, 0:count, :] = (keep_ref[k] + got_ref[k, 0:count, :].astype(F32)).astype(BF16)
        out_ref[k, count : count + EXTRA, 0:count] = packed
        out_ref[k, count : count + EXTRA, count:width] = jnp.zeros((EXTRA, width - count), BF16)


def output_kernel(got_ref, target_ref, out_ref, grad_ref, inverse_ref):
    count, width = target_ref.shape
    total = got_ref[0, 0:count, :].astype(F32)
    squares = unpack_rows(got_ref[0, count : count + EXTRA, 0:count])
    for k in range(1, NY):
        total = total + got_ref[k, 0:count, :].astype(F32)
        squares = squares + unpack_rows(got_ref[k, count : count + EXTRA, 0:count])
    inverse = lax.rsqrt(squares / FEATURES + EPSILON)
    inverse_ref[...] = jnp.broadcast_to(inverse, inverse_ref.shape)
    scale = as_columns(inverse)
    projected = total * jnp.concatenate([scale] * (width // HEAD_DIM), axis=1)
    out_ref[...] = projected.astype(BF16)
    grad = (projected - target_ref[...].astype(F32)).astype(BF16)
    grad_ref[0:count, :] = grad
    packed = pack_rows(row_sums(grad.astype(F32) * projected))
    grad_ref[count : count + EXTRA, 0:count] = packed
    grad_ref[count : count + EXTRA, count:width] = jnp.zeros((EXTRA, width - count), BF16)


def normed_grad_kernel(
    core, grad_ref, w0_ref, w1_ref, w3_ref, wa_ref, wb_ref, out_ref, inner_ref
):
    count, width = out_ref.shape[0], grad_ref.shape[2]
    x, c = lax.axis_index("x"), lax.axis_index("c")
    total = None
    for r, pair in enumerate(halves((w0_ref, w1_ref, w3_ref, wa_ref, wb_ref), c, width)):
        part = dot(grad_ref[lax.rem(x + r, NX), 0:count, :], pair[core](), 1, 0)
        total = part if total is None else total + part
    out_ref[...] = total
    inner = unpack_rows(grad_ref[0, count : count + EXTRA, 0:count])
    for k in range(1, NY):
        inner = inner + unpack_rows(grad_ref[k, count : count + EXTRA, 0:count])
    inner_ref[...] = jnp.broadcast_to(inner, inner_ref.shape)


def mixed_grad_kernel(
    part_ref, part_inner_ref, other_ref, w0_ref, w1_ref, w3_ref, wa_ref, wb_ref,
    mixed_ref, gain_ref, inverse_ref, q_ref, grad_ref, gain_grad_ref, state_ref,
):
    count = mixed_ref.shape[0]
    width = other_ref.shape[2]
    x, c = lax.axis_index("x"), lax.axis_index("c")
    total = part_ref[...]
    for r, (_, theirs) in enumerate(halves((w0_ref, w1_ref, w3_ref, wa_ref, wb_ref), c, width)):
        total = total + dot(other_ref[lax.rem(x + r, NX), 0:count, :], theirs(), 1, 0)
    inner = part_inner_ref[0:1, :]
    for k in range(NY):
        inner = inner + unpack_rows(other_ref[k, count : count + EXTRA, 0:count])
    inverse = inverse_ref[0:1, :]
    slope = inverse * inverse * inner / FEATURES
    heads = mixed_ref.shape[1] // HEAD_DIM
    scale = jnp.concatenate([as_columns(inverse)] * heads, axis=1)
    slope = jnp.concatenate([as_columns(slope)] * heads, axis=1)
    mixed = mixed_ref[...]
    scaled = scale * total
    grad = (gain_ref[...].astype(F32) * scaled - mixed * slope).astype(BF16)
    grad_ref[...] = grad
    gain_grad_ref[...] = jnp.sum(scaled * mixed, axis=0, keepdims=True)
    for h in range(heads):
        cols = head_cols(h)
        state_ref[cols, :] = dot(q_ref[:, cols], grad[:, cols], 0, 0).astype(BF16)


def weight_grad_kernel(own_ref, other_ref, mixed_ref, gain_ref, inverse_ref, out_ref):
    count = mixed_ref.shape[0]
    width = own_ref.shape[2]
    heads = mixed_ref.shape[1] // HEAD_DIM
    scale = jnp.concatenate([as_columns(inverse_ref[0:1, :])] * heads, axis=1)
    normed = (mixed_ref[...] * scale * gain_ref[...].astype(F32)).astype(BF16)
    turned = normed.T
    c = lax.axis_index("c")
    for k in range(NY):
        for ref, half in ((own_ref, c), (other_ref, 1 - c)):
            start = pl.multiple_of(k * NC * width + half * width, HEAD_DIM)
            out_ref[0, :, pl.ds(start, width)] = dot(turned, ref[k, 0:count, :], 1, 0).astype(BF16)


def local_grad_kernel(
    q_ref, k_ref, v_ref, grad_ref, state_ref, query_ref, key_ref, value_ref
):
    keep = keep_mask(q_ref.shape[0])
    for h in range(q_ref.shape[1] // HEAD_DIM):
        cols = head_cols(h)
        q, k, v, grad = q_ref[:, cols], k_ref[:, cols], v_ref[:, cols], grad_ref[:, cols]
        scores = jnp.where(keep, dot(q, k, 1, 1), 0.0).astype(BF16)
        pairs = jnp.where(keep, dot(grad, v, 1, 1), 0.0).astype(BF16)
        query = dot(pairs, k, 1, 0) + dot(grad, state_ref[cols, :], 1, 1)
        query_ref[:, cols] = query.astype(BF16)
        key_ref[:, cols] = dot(pairs, q, 0, 0)
        value_ref[:, cols] = dot(scores, grad, 0, 0)


def later_kernel(k_ref, v_ref, key_part_ref, value_part_ref, later_ref, key_ref, value_ref):
    for h in range(k_ref.shape[1] // HEAD_DIM):
        cols = head_cols(h)
        later = later_ref[cols, :]
        key_ref[:, cols] = (key_part_ref[:, cols] + dot(v_ref[:, cols], later, 1, 1)).astype(BF16)
        value = value_part_ref[:, cols] + dot(k_ref[:, cols], later, 1, 0)
        value_ref[:, cols] = value.astype(BF16)


def exchanged(blocks, axis):
    return lax.all_to_all(blocks, axis, 0, 0, tiled=True)


def carried(state, reverse):
    rows, cols = state.shape
    blocks = state.reshape(NZ, rows // NZ, cols)
    got = exchanged(blocks, "z")
    (totals,) = call(
        functools.partial(totals_kernel, reverse),
        [arr((NX, rows // NZ, cols), F32)], [got],
    )
    offsets = exchanged(totals, "x")
    (sums,) = call(
        functools.partial(prefix_kernel, reverse),
        [arr(blocks.shape, BF16)], [got, offsets],
    )
    return exchanged(sums, "z").reshape(rows, cols)


def ring(count, step):
    return [(i, (i + step) % count) for i in range(count)]


def work(queries, key_input, value_input, norm_gain, out_weight, target):
    count, feats = queries.shape
    width = target.shape[1]
    swap = [(0, 1), (1, 0)]
    gain = norm_gain.reshape(1, feats)
    mm = 2 * count * feats

    (state_local,) = call(
        state_kernel, [arr((feats, HEAD_DIM), BF16)], [key_input, value_input],
        mm * HEAD_DIM,
    )
    w0 = lax.all_gather(out_weight.T, "z", axis=0, tiled=True)
    w3 = lax.ppermute(w0, "x", ring(NX, 1))
    w1 = lax.ppermute(w0, "x", ring(NX, -1))
    wa = lax.ppermute(w3[:width], "x", ring(NX, 1))
    wb = lax.ppermute(w1[width:], "x", ring(NX, -1))
    weights = [w0, w1, w3, wa, wb]

    (attended,) = call(
        local_kernel, [arr((count, feats), F32)], [queries, key_input, value_input],
        2 * mm * count,
    )
    state_low = carried(state_local, False)
    message = (NY, count + EXTRA, width)
    columns = NY * NC * width
    mixed, scaled, sent, sums = call(
        project_kernel,
        [
            arr((count, feats), F32),
            arr((count, feats), BF16),
            arr(message, BF16),
            arr((EXTRA, count), F32),
        ],
        [attended, queries, state_low, gain, *weights],
        mm * (HEAD_DIM + columns // 2),
    )
    (kept,) = call(
        project_own_kernel, [arr((NY, count, width), F32)], [scaled, *weights],
        mm * columns // 2,
    )
    got = lax.ppermute(sent, "c", swap)
    (paired,) = call(pair_kernel, [arr(message, BF16)], [kept, got, sums])
    arrived = exchanged(paired, "y")
    output, grad_local, inverse = call(
        output_kernel,
        [
            arr((count, width), BF16),
            arr((count + EXTRA, width), BF16),
            arr((EXTRA, count), F32),
        ],
        [arrived, target],
    )
    own = lax.all_gather(grad_local, "y", axis=0, tiled=True).reshape(message)
    other = lax.ppermute(own, "c", swap)
    part, part_inner = call(
        functools.partial(normed_grad_kernel, 0),
        [arr((count, feats), F32), arr((EXTRA, count), F32)], [own, *weights],
        mm * columns // 2,
    )
    mixed_grad, gain_grads, grad_state = call(
        mixed_grad_kernel,
        [arr((count, feats), BF16), arr((1, feats), F32), arr((feats, HEAD_DIM), BF16)],
        [part, part_inner, other, *weights, mixed, gain, inverse, queries],
        mm * (HEAD_DIM + columns // 2),
    )
    (weight_grads,) = call(
        weight_grad_kernel, [arr((1, feats, columns), BF16)],
        [own, other, mixed, gain, inverse], mm * columns, 60 << 20,
    )
    query_grad, key_part, value_part = call(
        local_grad_kernel,
        [arr((count, feats), BF16), arr((count, feats), F32), arr((count, feats), F32)],
        [queries, key_input, value_input, mixed_grad, state_low],
        mm * (5 * count + HEAD_DIM), 60 << 20,
    )
    later_low = carried(grad_state, True)
    key_grad, value_grad = call(
        later_kernel, [arr((count, feats), BF16)] * 2,
        [key_input, value_input, key_part, value_part, later_low], 2 * mm * HEAD_DIM,
    )
    return output, query_grad, key_grad, value_grad, gain_grads, weight_grads


def solution(mesh):
    torus = Mesh(mesh.devices.reshape(NX, NZ, NY, NC), ("x", "z", "y", "c"))
    return jax.shard_map(
        work,
        mesh=torus,
        in_specs=(
            P(SEQ, HEAD),
            P(SEQ, HEAD),
            P(SEQ, HEAD),
            P(HEAD),
            P(HEAD, SEQ),
            P(SEQ, HEAD),
        ),
        out_specs=(
            P(SEQ, HEAD),
            P(SEQ, HEAD),
            P(SEQ, HEAD),
            P(SEQ, HEAD),
            P(SEQ, HEAD),
            P(SEQ, HEAD, None),
        ),
        check_vma=False,
    )
```

```python
import jax
import jax.numpy as jnp
from jax import lax
from jax.experimental import pallas as pl
from jax.experimental.pallas import tpu as pltpu
from jax.sharding import Mesh
from jax.sharding import PartitionSpec as P


HEAD_DIM = 128
FEATURES = 4096
SEQ = ("x", "zh", "zl")
Z = ("zh", "zl")
NEAR = ("x", "zl")
HEAD = ("y", "c")
EPSILON = 1e-06
F32 = jnp.float32
BF16 = jnp.bfloat16
NX, NZ, NY, NC = 4, 16, 4, 2
FAR = 4
VMEM_LIMIT = 16 << 20
EXTRA = 8


def dot(a, b, ca, cb):
    return lax.dot_general(a, b, (((ca,), (cb,)), ((), ())), preferred_element_type=F32)


def call(kernel, outs, args, flops=0, vmem=VMEM_LIMIT):
    moved = sum(a.size * a.dtype.itemsize for a in args)
    moved += sum(o.size * o.dtype.itemsize for o in outs)
    return pl.pallas_call(
        kernel,
        out_shape=outs,
        in_specs=[pl.BlockSpec(memory_space=pltpu.VMEM)] * len(args),
        out_specs=[pl.BlockSpec(memory_space=pltpu.VMEM)] * len(outs),
        cost_estimate=pl.CostEstimate(flops=flops, bytes_accessed=moved, transcendentals=0),
        compiler_params=pltpu.CompilerParams(vmem_limit_bytes=vmem),
    )(*args)


def arr(shape, dtype):
    return jax.ShapeDtypeStruct(shape, dtype)


def head_cols(h):
    return slice(h * HEAD_DIM, (h + 1) * HEAD_DIM)


def keep_mask(count):
    rows = lax.broadcasted_iota(jnp.int32, (count, count), 0)
    cols = lax.broadcasted_iota(jnp.int32, (count, count), 1)
    return rows >= cols


def row_sums(p):
    high = p.astype(BF16)
    low = (p - high.astype(F32)).astype(BF16)
    ones = jnp.ones((EXTRA, p.shape[1]), BF16)
    return dot(ones, high, 1, 1) + dot(ones, low, 1, 1)


def pack_rows(sums):
    high = sums.astype(BF16).astype(F32)
    low = sums - high
    row = lax.broadcasted_iota(jnp.int32, sums.shape, 0)
    return jnp.where(row < EXTRA // 2, high, low).astype(BF16)


def unpack_rows(packed):
    wide = packed.astype(F32)
    return wide[0:1] + wide[EXTRA // 2 : EXTRA // 2 + 1]


def as_columns(row):
    return jnp.broadcast_to(row, (HEAD_DIM, row.shape[1])).T


def state_kernel(a_ref, b_ref, out_ref):
    for h in range(a_ref.shape[1] // HEAD_DIM):
        cols = head_cols(h)
        out_ref[cols, :] = dot(a_ref[:, cols], b_ref[:, cols], 0, 0).astype(BF16)


def local_kernel(q_ref, k_ref, v_ref, out_ref):
    keep = keep_mask(q_ref.shape[0])
    for h in range(q_ref.shape[1] // HEAD_DIM):
        cols = head_cols(h)
        scores = dot(q_ref[:, cols], k_ref[:, cols], 1, 1)
        scores = jnp.where(keep, scores, 0.0).astype(BF16)
        out_ref[:, cols] = dot(scores, v_ref[:, cols], 1, 0)


def totals_kernel(in_ref, out_ref):
    total = in_ref[0].astype(F32)
    for i in range(1, NZ):
        total = total + in_ref[i].astype(F32)
    x = lax.axis_index("x")
    for k in range(NX):
        out_ref[k] = jnp.where(k > x, total, 0.0)


def prefix_kernel(in_ref, offset_ref, out_ref):
    running = offset_ref[0]
    for k in range(1, NX):
        running = running + offset_ref[k]
    for i in range(NZ):
        out_ref[i] = running.astype(BF16)
        running = running + in_ref[i].astype(F32)


def halves(refs, c, width):
    w0_ref, w1_ref, w3_ref, wa_ref, wb_ref = refs
    own = pl.ds(pl.multiple_of(c * width, width), width)
    other = pl.ds(pl.multiple_of((1 - c) * width, width), width)
    first, second = wa_ref[...], wb_ref[...]
    return (
        (lambda: w0_ref[own, :], lambda: w0_ref[other, :]),
        (lambda: w1_ref[own, :], lambda: w1_ref[other, :]),
        (lambda: jnp.where(c == 0, first, second), lambda: jnp.where(c == 0, second, first)),
        (lambda: w3_ref[own, :], lambda: w3_ref[other, :]),
    )


def group_totals_kernel(in_ref, out_ref):
    near = NZ // FAR
    rows = in_ref.shape[1]
    for x in range(NX):
        total = in_ref[x * near].astype(F32)
        for i in range(1, near):
            total = total + in_ref[x * near + i].astype(F32)
        for k in range(FAR):
            out_ref[k, x * rows : (x + 1) * rows, :] = total.astype(BF16)


def suffix_kernel(in_ref, groups_ref, out_ref):
    near = NZ // FAR
    rows = in_ref.shape[1]
    me = lax.axis_index("zh")
    carry = jnp.zeros(in_ref.shape[1:], F32)
    for x in reversed(range(NX)):
        running = carry
        for k in range(FAR):
            group = groups_ref[k, x * rows : (x + 1) * rows, :].astype(F32)
            running = running + jnp.where(k > me, group, 0.0)
            carry = carry + group
        for i in reversed(range(near)):
            out_ref[x * near + i] = running.astype(BF16)
            running = running + in_ref[x * near + i].astype(F32)


def project_kernel(
    att_ref, q_ref, state_ref, gain_ref, w0_ref, w1_ref, w3_ref, wa_ref, wb_ref,
    mixed_ref, scaled_ref, send_ref, sums_ref,
):
    for h in range(q_ref.shape[1] // HEAD_DIM):
        cols = head_cols(h)
        mixed_ref[:, cols] = att_ref[:, cols] + dot(q_ref[:, cols], state_ref[cols, :], 1, 0)
    mixed = mixed_ref[...]
    scaled = (mixed * gain_ref[...].astype(F32)).astype(BF16)
    scaled_ref[...] = scaled
    sums = row_sums(mixed * mixed)
    sums_ref[...] = sums
    packed = pack_rows(sums)
    x, c = lax.axis_index("x"), lax.axis_index("c")
    count, width = mixed.shape[0], send_ref.shape[2]
    for r, (_, theirs) in enumerate(halves((w0_ref, w1_ref, w3_ref, wa_ref, wb_ref), c, width)):
        place = lax.rem(x + r, NX)
        send_ref[place, 0:count, :] = dot(scaled, theirs(), 1, 1).astype(BF16)
        send_ref[r, count : count + EXTRA, 0:count] = packed
        send_ref[r, count : count + EXTRA, count:width] = jnp.zeros((EXTRA, width - count), BF16)


def project_own_kernel(scaled_ref, w0_ref, w1_ref, w3_ref, wa_ref, wb_ref, keep_ref):
    x, c = lax.axis_index("x"), lax.axis_index("c")
    width = keep_ref.shape[2]
    scaled = scaled_ref[...]
    for r, (mine, _) in enumerate(halves((w0_ref, w1_ref, w3_ref, wa_ref, wb_ref), c, width)):
        keep_ref[lax.rem(x + r, NX)] = dot(scaled, mine(), 1, 1)


def pair_kernel(keep_ref, got_ref, sums_ref, out_ref):
    count, width = keep_ref.shape[1], keep_ref.shape[2]
    sums = sums_ref[...] + unpack_rows(got_ref[0, count : count + EXTRA, 0:count])
    packed = pack_rows(sums)
    for k in range(NY):
        out_ref[k, 0:count, :] = (keep_ref[k] + got_ref[k, 0:count, :].astype(F32)).astype(BF16)
        out_ref[k, count : count + EXTRA, 0:count] = packed
        out_ref[k, count : count + EXTRA, count:width] = jnp.zeros((EXTRA, width - count), BF16)


def output_kernel(got_ref, target_ref, out_ref, grad_ref, inverse_ref):
    count, width = target_ref.shape
    total = got_ref[0, 0:count, :].astype(F32)
    squares = unpack_rows(got_ref[0, count : count + EXTRA, 0:count])
    for k in range(1, NY):
        total = total + got_ref[k, 0:count, :].astype(F32)
        squares = squares + unpack_rows(got_ref[k, count : count + EXTRA, 0:count])
    inverse = lax.rsqrt(squares / FEATURES + EPSILON)
    inverse_ref[...] = jnp.broadcast_to(inverse, inverse_ref.shape)
    scale = as_columns(inverse)
    projected = total * jnp.concatenate([scale] * (width // HEAD_DIM), axis=1)
    out_ref[...] = projected.astype(BF16)
    grad = (projected - target_ref[...].astype(F32)).astype(BF16)
    grad_ref[0:count, :] = grad
    packed = pack_rows(row_sums(grad.astype(F32) * projected))
    grad_ref[count : count + EXTRA, 0:count] = packed
    grad_ref[count : count + EXTRA, count:width] = jnp.zeros((EXTRA, width - count), BF16)


def normed_grad_kernel(
    grad_ref, w0_ref, w1_ref, w3_ref, wa_ref, wb_ref, out_ref, inner_ref
):
    count, width = out_ref.shape[0], grad_ref.shape[2]
    x, c = lax.axis_index("x"), lax.axis_index("c")
    total = None
    for r, pair in enumerate(halves((w0_ref, w1_ref, w3_ref, wa_ref, wb_ref), c, width)):
        part = dot(grad_ref[lax.rem(x + r, NX), 0:count, :], pair[0](), 1, 0)
        total = part if total is None else total + part
    out_ref[...] = total
    inner = unpack_rows(grad_ref[0, count : count + EXTRA, 0:count])
    for k in range(1, NY):
        inner = inner + unpack_rows(grad_ref[k, count : count + EXTRA, 0:count])
    inner_ref[...] = jnp.broadcast_to(inner, inner_ref.shape)


def mixed_grad_kernel(
    part_ref, part_inner_ref, other_ref, w0_ref, w1_ref, w3_ref, wa_ref, wb_ref,
    mixed_ref, gain_ref, inverse_ref, q_ref, grad_ref, gain_grad_ref, state_ref,
):
    count = mixed_ref.shape[0]
    width = other_ref.shape[2]
    x, c = lax.axis_index("x"), lax.axis_index("c")
    total = part_ref[...]
    for r, (_, theirs) in enumerate(halves((w0_ref, w1_ref, w3_ref, wa_ref, wb_ref), c, width)):
        total = total + dot(other_ref[lax.rem(x + r, NX), 0:count, :], theirs(), 1, 0)
    inner = part_inner_ref[0:1, :]
    for k in range(NY):
        inner = inner + unpack_rows(other_ref[k, count : count + EXTRA, 0:count])
    inverse = inverse_ref[0:1, :]
    slope = inverse * inverse * inner / FEATURES
    heads = mixed_ref.shape[1] // HEAD_DIM
    scale = jnp.concatenate([as_columns(inverse)] * heads, axis=1)
    slope = jnp.concatenate([as_columns(slope)] * heads, axis=1)
    mixed = mixed_ref[...]
    scaled = scale * total
    grad = (gain_ref[...].astype(F32) * scaled - mixed * slope).astype(BF16)
    grad_ref[...] = grad
    gain_grad_ref[...] = jnp.sum(scaled * mixed, axis=0, keepdims=True)
    for h in range(heads):
        cols = head_cols(h)
        state_ref[cols, :] = dot(q_ref[:, cols], grad[:, cols], 0, 0).astype(BF16)


def weight_grad_kernel(own_ref, other_ref, mixed_ref, gain_ref, inverse_ref, out_ref):
    count = mixed_ref.shape[0]
    width = own_ref.shape[2]
    heads = mixed_ref.shape[1] // HEAD_DIM
    scale = jnp.concatenate([as_columns(inverse_ref[0:1, :])] * heads, axis=1)
    normed = (mixed_ref[...] * scale * gain_ref[...].astype(F32)).astype(BF16)
    turned = normed.T
    c = lax.axis_index("c")
    for k in range(NY):
        for ref, half in ((own_ref, c), (other_ref, 1 - c)):
            start = pl.multiple_of(k * NC * width + half * width, HEAD_DIM)
            out_ref[0, :, pl.ds(start, width)] = dot(turned, ref[k, 0:count, :], 1, 0).astype(BF16)


def local_grad_kernel(
    q_ref, k_ref, v_ref, grad_ref, state_ref, query_ref, key_ref, value_ref
):
    keep = keep_mask(q_ref.shape[0])
    for h in range(q_ref.shape[1] // HEAD_DIM):
        cols = head_cols(h)
        q, k, v, grad = q_ref[:, cols], k_ref[:, cols], v_ref[:, cols], grad_ref[:, cols]
        scores = jnp.where(keep, dot(q, k, 1, 1), 0.0).astype(BF16)
        pairs = jnp.where(keep, dot(grad, v, 1, 1), 0.0).astype(BF16)
        query = dot(pairs, k, 1, 0) + dot(grad, state_ref[cols, :], 1, 1)
        query_ref[:, cols] = query.astype(BF16)
        key_ref[:, cols] = dot(pairs, q, 0, 0)
        value_ref[:, cols] = dot(scores, grad, 0, 0)


def later_kernel(k_ref, v_ref, key_part_ref, value_part_ref, later_ref, key_ref, value_ref):
    for h in range(k_ref.shape[1] // HEAD_DIM):
        cols = head_cols(h)
        later = later_ref[cols, :]
        key_ref[:, cols] = (key_part_ref[:, cols] + dot(v_ref[:, cols], later, 1, 1)).astype(BF16)
        value = value_part_ref[:, cols] + dot(k_ref[:, cols], later, 1, 0)
        value_ref[:, cols] = value.astype(BF16)


def exchanged(blocks, axis):
    return lax.all_to_all(blocks, axis, 0, 0, tiled=True)


def carried(state):
    rows, cols = state.shape
    blocks = state.reshape(NZ, rows // NZ, cols)
    got = exchanged(blocks, Z)
    (totals,) = call(
        totals_kernel,
        [arr((NX, rows // NZ, cols), F32)], [got],
    )
    offsets = exchanged(totals, "x")
    (sums,) = call(
        prefix_kernel,
        [arr(blocks.shape, BF16)], [got, offsets],
    )
    return exchanged(sums, Z).reshape(rows, cols)


def carried_back(state):
    rows, cols = state.shape
    blocks = state.reshape(NZ, rows // NZ, cols)
    got = exchanged(blocks, NEAR)
    (totals,) = call(group_totals_kernel, [arr((FAR, NX * (rows // NZ), cols), BF16)], [got])
    groups = exchanged(totals, "zh")
    (sums,) = call(suffix_kernel, [arr(blocks.shape, BF16)], [got, groups])
    return exchanged(sums, NEAR).reshape(rows, cols)


def ring(count, step):
    return [(i, (i + step) % count) for i in range(count)]


def work(queries, key_input, value_input, norm_gain, out_weight, target):
    count, feats = queries.shape
    width = target.shape[1]
    swap = [(0, 1), (1, 0)]
    gain = norm_gain.reshape(1, feats)
    mm = 2 * count * feats

    (state_local,) = call(
        state_kernel, [arr((feats, HEAD_DIM), BF16)], [key_input, value_input],
        mm * HEAD_DIM, 60 << 20,
    )
    w0 = lax.all_gather(out_weight.T, Z, axis=0, tiled=True)
    w3 = lax.ppermute(w0, "x", ring(NX, 1))
    w1 = lax.ppermute(w0, "x", ring(NX, -1))
    wa = lax.ppermute(w3[:width], "x", ring(NX, 1))
    wb = lax.ppermute(w1[width:], "x", ring(NX, -1))
    weights = [w0, w1, w3, wa, wb]

    (attended,) = call(
        local_kernel, [arr((count, feats), F32)], [queries, key_input, value_input],
        2 * mm * count, 60 << 20,
    )
    state_low = carried(state_local)
    message = (NY, count + EXTRA, width)
    columns = NY * NC * width
    mixed, scaled, sent, sums = call(
        project_kernel,
        [
            arr((count, feats), F32),
            arr((count, feats), BF16),
            arr(message, BF16),
            arr((EXTRA, count), F32),
        ],
        [attended, queries, state_low, gain, *weights],
        mm * (HEAD_DIM + columns // 2),
    )
    (kept,) = call(
        project_own_kernel, [arr((NY, count, width), F32)], [scaled, *weights],
        mm * columns // 2,
    )
    got = lax.ppermute(sent, "c", swap)
    (paired,) = call(pair_kernel, [arr(message, BF16)], [kept, got, sums])
    arrived = exchanged(paired, "y")
    output, grad_local, inverse = call(
        output_kernel,
        [
            arr((count, width), BF16),
            arr((count + EXTRA, width), BF16),
            arr((EXTRA, count), F32),
        ],
        [arrived, target],
    )
    own = lax.all_gather(grad_local, "y", axis=0, tiled=True).reshape(message)
    other = lax.ppermute(own, "c", swap)
    part, part_inner = call(
        normed_grad_kernel,
        [arr((count, feats), F32), arr((EXTRA, count), F32)], [own, *weights],
        mm * columns // 2,
    )
    mixed_grad, gain_grads, grad_state = call(
        mixed_grad_kernel,
        [arr((count, feats), BF16), arr((1, feats), F32), arr((feats, HEAD_DIM), BF16)],
        [part, part_inner, other, *weights, mixed, gain, inverse, queries],
        mm * (HEAD_DIM + columns // 2),
    )
    (weight_grads,) = call(
        weight_grad_kernel, [arr((1, feats, columns), BF16)],
        [own, other, mixed, gain, inverse], mm * columns, 60 << 20,
    )
    query_grad, key_part, value_part = call(
        local_grad_kernel,
        [arr((count, feats), BF16), arr((count, feats), F32), arr((count, feats), F32)],
        [queries, key_input, value_input, mixed_grad, state_low],
        mm * (5 * count + HEAD_DIM), 60 << 20,
    )
    later_low = carried_back(grad_state)
    key_grad, value_grad = call(
        later_kernel, [arr((count, feats), BF16)] * 2,
        [key_input, value_input, key_part, value_part, later_low], 2 * mm * HEAD_DIM,
    )
    return output, query_grad, key_grad, value_grad, gain_grads, weight_grads


def solution(mesh):
    torus = Mesh(mesh.devices.reshape(NX, FAR, NZ // FAR, NY, NC), ("x", "zh", "zl", "y", "c"))
    return jax.shard_map(
        work,
        mesh=torus,
        in_specs=(
            P(SEQ, HEAD),
            P(SEQ, HEAD),
            P(SEQ, HEAD),
            P(HEAD),
            P(HEAD, SEQ),
            P(SEQ, HEAD),
        ),
        out_specs=(
            P(SEQ, HEAD),
            P(SEQ, HEAD),
            P(SEQ, HEAD),
            P(SEQ, HEAD),
            P(SEQ, HEAD),
            P(SEQ, HEAD, None),
        ),
        check_vma=False,
    )
```
